32 devices in a mesh: row: 4 (over y, x), col: 8 (over z, core).
Axes of the slice: x: 2, y: 2, z: 4, core: 2. Of those that a mesh axis runs over, the one named last changes fastest.
Arguments:
- velocity: float32 [3, 8, 8, 36, 32, 512], P(None, 'col', 'row'), may hold values from -6 to 6
- y_sizes: int32 [8], replicated, may hold values from 1 to 36, 256 in all
- old_place: int32 [8, 8], replicated, may hold values from 0 to 7, each once within a row
- new_col: int32 [8, 8], replicated, may hold values from 0 to 7, each once within a row
Outputs:
- divergence: float32 [8, 8, 4, 256, 512], P('row', 'col')
- peak: float32 [256, 512], replicated
The draws below stay inside these ranges and needn't reach their ends.
Inputs may be any that keep to these rules, and one draw needn't show every extreme that they name: `y_sizes`: the heights sum to 256 and the tallest is exactly 36. `old_place`: each row is a permutation of 0 to 7. `new_col`: each row is a permutation of 0 to 8 - 1.
All inputs are finite; a program needn't handle non-finite values.
Results may differ from the reference program's by a relative error of at most 0.0003.
Values sent between devices are 32-bit elements; how exact they have to be, the bound alone decides.
A program may use at most 320 MiB of HBM per device.

```python
import math
import jax
import jax.numpy as jnp
import numpy as np
from jax import lax

NX = 512
ZB = 32
YCAP = 36
NBZ = 8
NBY = 8
NY = 256
N_COL = 8


def block_levels(own_key, dims, pieces, low, top_value):
    def one(axis_at, blocks):
        heights = jax.random.uniform(jax.random.fold_in(jax.random.fold_in(own_key, 6), axis_at), (blocks,), jnp.float32, low / len(pieces), top_value / len(pieces))
        return jnp.repeat(jnp.exp(heights), dims[axis_at] // blocks).reshape((-1,) + (1,) * (len(dims) - axis_at - 1))

    gain = one(*pieces[0])
    for cut in pieces[1:]:
        gain = gain * one(*cut)
    return gain


def split_up(amount, total, limit, slope):
    portions = [(1 << 20) // math.isqrt(grade ** slope) + 1 for grade in range(2, amount + 1)]
    rest, given = total - limit - (amount - 1), [1] * (amount - 1)
    while rest > 0:
        candidates = [i for i in range(amount - 1) if given[i] < limit]
        mass, budget = sum([portions[i] for i in candidates]), rest
        for i in candidates:
            more = min(limit - given[i], max(1, budget * portions[i] // mass), rest)
            given[i] = given[i] + more
            rest = rest - more
    return np.array([limit] + given)


def ragged_sizes(key, amount, total, most, slope):
    if amount == 2:
        one = jax.random.randint(key, (), max(1, total - most), min(most, total - 1) + 1)
        return jnp.stack([one, total - one])
    sizes = jnp.asarray(split_up(amount, total, most, slope), jnp.int32)
    twos = (amount - 1) // 2
    donor, receiver = sizes[1:1 + 2 * twos:2], sizes[2:2 + 2 * twos:2]
    slack = jnp.minimum(donor - 1, most - receiver)
    moved = jax.random.randint(jax.random.fold_in(key, 1), (twos,), 0, 1 << 20) % (slack + 1)
    sizes = sizes.at[1:1 + 2 * twos:2].set(donor - moved).at[2:2 + 2 * twos:2].set(receiver + moved)
    return sizes[jax.random.permutation(jax.random.fold_in(key, 2), amount)]


def normal_values(stream_key, extent, scale, most, cuts=(), kind=jnp.bfloat16):
    loudness = block_levels(stream_key, extent, cuts, -0.22, 0.18) if cuts else 1.0
    drawn = jax.random.normal(stream_key, extent, jnp.float32) * scale * loudness
    return jnp.minimum(jnp.maximum(drawn, -most), most).astype(kind)


def setup_inputs(seed: int = 0) -> dict:
    key_of = jax.random.split(jax.random.key(seed), 5)
    velocity = normal_values(key_of[0], (3, NBZ, NBY, YCAP, ZB, NX), 1.0, 6.0, ((1, 8), (2, 4)), jnp.float32)
    y_sizes = ragged_sizes(key_of[1], NBY, NY, YCAP, 1).astype(jnp.int32)
    old_place = jax.vmap(lambda own: jax.random.permutation(own, NBY))(jax.random.split(key_of[2], NBZ)).reshape((NBZ, NBY)).astype(jnp.int32)
    new_col = jax.vmap(lambda own: jax.random.permutation(own, N_COL))(jax.random.split(key_of[3], NBZ)).reshape((NBZ, N_COL)).astype(jnp.int32)
    return {"velocity": velocity, "y_sizes": y_sizes, "old_place": old_place, "new_col": new_col}


def derive(field, axis):
    count = field.shape[axis]
    spectrum = jnp.fft.rfft(field, axis=axis)
    modes = jnp.arange(count // 2 + 1)
    wave = jnp.where(modes == count // 2, 0, modes).astype(field.dtype) * (4.0 / count)
    shape = [1] * field.ndim
    shape[axis] = count // 2 + 1
    spectrum = spectrum * (1j * wave.reshape(shape))
    return jnp.fft.irfft(spectrum, n=count, axis=axis).astype(field.dtype)


def source_rows(y_sizes, old_place, row_depth, height):
    ends = jnp.cumsum(y_sizes).astype(jnp.int32)
    starts = (ends - y_sizes).astype(jnp.int32)
    cells = jnp.arange(height, dtype=jnp.int32)
    block = jnp.sum((cells[:, None] >= ends[None, :]).astype(jnp.int32), axis=1).astype(jnp.int32)
    offset = cells - jnp.take(starts, block)
    return (jnp.take(old_place, block, axis=1) * row_depth + offset).astype(jnp.int32)


def assemble(pair):
    block, index = pair
    flat = block.reshape(-1, block.shape[2], block.shape[3])
    return jnp.transpose(jnp.take(flat, index, axis=0), (1, 0, 2))


def reference(velocity, y_sizes, old_place, new_col):
    row_depth = velocity.shape[3]
    rows = source_rows(y_sizes, old_place, row_depth, NY)
    vertical = lax.map(assemble, (velocity[2], rows)).reshape(-1, NY, NX)
    slope_z = derive(vertical, 0).reshape(N_COL, ZB, NY, NX)

    def combine(group):
        block_x, block_y, index, part_z = group
        slope_x = derive(assemble((block_x, index)), 2)
        slope_y = derive(assemble((block_y, index)), 1)
        return slope_x + slope_y + part_z

    field = lax.map(combine, (velocity[0], velocity[1], rows, slope_z))
    peak = jnp.max(jnp.abs(field), axis=(0, 1))
    field = field.reshape(N_COL, N_COL, ZB // N_COL, NY, NX)
    hits = (new_col[:, :, None] == jnp.arange(N_COL, dtype=jnp.int32)[None, None, :]).astype(jnp.int32)
    slab_of = jnp.sum(hits * jnp.arange(N_COL, dtype=jnp.int32)[None, :, None], axis=1).astype(jnp.int32)
    divergence = jnp.take_along_axis(field, slab_of[:, :, None, None, None], axis=1)
    return (divergence, peak)
```

```python
import math

import jax
import jax.numpy as jnp
from jax import lax
from jax.sharding import PartitionSpec as P

YMEAN = 32


FINE = lax.Precision.HIGH


def spectral_matrix(to, source, count):
    gap = (to[:, None] - source[None, :]) % count
    angle = gap.astype(jnp.float32) * (math.pi / count)
    parity = 1.0 - 2.0 * (gap % 2).astype(jnp.float32)
    divisor = jnp.where(gap == 0, 1.0, jnp.sin(angle))
    return jnp.where(gap == 0, 0.0, parity * jnp.cos(angle) / divisor * (2.0 / count))


def source_rows(y_sizes, place, row_depth, height):
    ends = jnp.cumsum(y_sizes)
    starts = ends - y_sizes
    cells = jnp.arange(height, dtype=jnp.int32)
    block = jnp.sum((cells[:, None] >= ends[None, :]).astype(jnp.int32), axis=1)
    stored = jnp.take(place, block) * row_depth + cells - jnp.take(starts, block)
    return stored


def row_exchange(value, split, concat):
    return lax.all_to_all(value, "row", split_axis=split, concat_axis=concat, tiled=True)


def col_exchange(value, split, concat):
    return lax.all_to_all(value, "col", split_axis=split, concat_axis=concat, tiled=True)


def on_device(velocity, y_sizes, old_place, new_col):
    velocity = velocity[:, 0]
    fields, places, row_depth, planes, x_cells = velocity.shape
    columns = lax.axis_size("col")
    rows_count = lax.axis_size("row")
    my_col = lax.axis_index("col")
    thick = planes // columns
    blocks_y = y_sizes.shape[0]
    height = YMEAN * blocks_y
    depth = planes * columns
    x_part = x_cells // rows_count
    y_part = height // columns
    slots = jnp.arange(columns, dtype=jnp.int32)
    hits = (new_col[:, :, None] == slots[None, None, :]).astype(jnp.int32)
    slab_of = jnp.sum(hits * slots[None, :, None], axis=1)

    stored = source_rows(y_sizes, jnp.take(old_place, my_col, axis=0), row_depth, height)
    pick = (stored[:, None] == jnp.arange(blocks_y * row_depth)[None, :]).astype(jnp.float32)
    cells = jnp.arange(height, dtype=jnp.int32)
    grid_row = jnp.sum(pick * cells[:, None].astype(jnp.float32), axis=0).astype(jnp.int32)
    used = jnp.sum(pick, axis=0)
    across_y = spectral_matrix(cells, grid_row, height) * used[None, :]
    steps_x = jnp.arange(x_cells, dtype=jnp.int32)
    across_x = spectral_matrix(steps_x, steps_x, x_cells)

    slope_x = jnp.dot(velocity[0], across_x.T, precision=FINE, preferred_element_type=jnp.float32)
    along_y = jnp.stack([slope_x, velocity[1]])
    two = row_exchange(along_y, 4, 1)
    third = row_exchange(velocity[2], 3, 0)
    two = two.reshape(2, blocks_y * row_depth, planes, x_part)
    third = third.reshape(blocks_y * row_depth, planes, x_part)
    upright = jnp.take(third, stored, axis=0)
    upright = col_exchange(upright.reshape(columns, y_part, planes, x_part), 0, 0)
    first = slots[None, :, None] * planes + slab_of.T[:, :, None] * thick
    targets = (first + jnp.arange(thick, dtype=jnp.int32)).reshape(-1)
    across_z = spectral_matrix(targets, jnp.arange(depth, dtype=jnp.int32), depth)
    slope_z = jnp.einsum(
        "akz,kyzx->ayx",
        across_z.reshape(depth, columns, planes),
        upright,
        precision=FINE,
    )
    slope_z = slope_z.reshape(columns, planes, y_part, x_part)
    slope_z = lax.all_to_all(
        slope_z, "col", split_axis=0, concat_axis=2, tiled=True
    ).reshape(planes, height, x_part)
    flat = jnp.einsum("jy,yzx->zjx", across_y, two[1], precision=FINE)
    flat = flat + jnp.swapaxes(jnp.take(two[0], stored, axis=0), 0, 1)
    flat = flat.reshape(columns, thick, height, x_part)
    flat = jnp.take(flat, jnp.take(slab_of, my_col, axis=0), axis=0)
    flat = col_exchange(flat, 0, 0).reshape(planes, height, x_part)
    part = flat + slope_z
    local_peak = jnp.max(jnp.abs(part), axis=0)
    peak = lax.pmax(local_peak, "col")
    peak = lax.all_gather(peak, "row", axis=1, tiled=True)
    field = row_exchange(part, 0, 2)
    field = field.reshape(columns // rows_count, 1, thick, height, x_cells)
    return (field, peak)


def solution(mesh):
    in_specs = (P(None, "col", "row", None, None, None), P(), P(), P())
    out_specs = (P("row", "col", None, None, None), P())
    return jax.shard_map(
        on_device, mesh=mesh, in_specs=in_specs, out_specs=out_specs, check_vma=False
    )
```

```python
import functools
import math

import jax
import jax.numpy as jnp
from jax import lax
from jax.experimental import pallas as pl
from jax.experimental.pallas import tpu as pltpu
from jax.sharding import PartitionSpec as P

YMEAN = 32


FINE = lax.Precision.HIGH

LANES = 128


def exchange_kernel(jobs, sizes, count_in, count_out, *refs):
    ins, outs = refs[:count_in], refs[count_in : count_in + count_out]
    rest = refs[count_in + count_out :]
    held, (send_sem, recv_sem, in_sem, out_sem) = rest[: len(jobs)], rest[len(jobs) :]
    barrier = pltpu.get_barrier_semaphore()
    greeted = 0
    for axis in sorted({job[2] for job in jobs}):
        me = lax.axis_index(axis)
        for step in range(1, sizes[axis]):
            partner = lax.rem(me + step, sizes[axis])
            pl.semaphore_signal(
                barrier, inc=1, device_id={axis: partner}, device_id_type=pl.DeviceIdType.MESH
            )
            greeted += 1
    pl.semaphore_wait(barrier, greeted)
    copies, own = [], []
    at = 0
    for number, (source, target, axis, pick, put) in enumerate(jobs):
        size = sizes[axis]
        me = lax.axis_index(axis)
        for step in range(1, size):
            partner = lax.rem(me + step, size)
            copy = pltpu.make_async_remote_copy(
                src_ref=pick(ins[source], partner),
                dst_ref=put(outs[target], me),
                send_sem=send_sem.at[at],
                recv_sem=recv_sem.at[at],
                device_id={axis: partner},
                device_id_type=pl.DeviceIdType.MESH,
            )
            copy.start()
            copies.append(copy)
            at += 1
    for number, (source, target, axis, pick, put) in enumerate(jobs):
        me = lax.axis_index(axis)
        copy = pltpu.make_async_copy(pick(ins[source], me), held[number], in_sem.at[number])
        copy.start()
        own.append(copy)
    last = []
    for number, (source, target, axis, pick, put) in enumerate(jobs):
        me = lax.axis_index(axis)
        own[number].wait()
        copy = pltpu.make_async_copy(held[number], put(outs[target], me), out_sem.at[number])
        copy.start()
        last.append(copy)
    for copy in last:
        copy.wait()
    for copy in copies:
        copy.wait()


def exchange(number, inputs, outputs, jobs, blocks):
    sizes = {axis: lax.axis_size(axis) for axis in ("row", "col")}
    total = sum(sizes[job[2]] - 1 for job in jobs)
    dma = pltpu.SemaphoreType.DMA
    return pl.pallas_call(
        functools.partial(exchange_kernel, jobs, sizes, len(inputs), len(outputs)),
        out_shape=[jax.ShapeDtypeStruct(shape, jnp.float32) for shape in outputs],
        in_specs=[pl.BlockSpec(memory_space=pl.ANY)] * len(inputs),
        out_specs=[pl.BlockSpec(memory_space=pl.ANY)] * len(outputs),
        scratch_shapes=[pltpu.VMEM(block, jnp.float32) for block in blocks]
        + [dma((total,)), dma((total,)), dma((len(jobs),)), dma((len(jobs),))],
        compiler_params=pltpu.CompilerParams(collective_id=number, has_side_effects=True),
        name=f"exchange{number}",
    )(*inputs)


def lanes(part):
    return pl.ds(pl.multiple_of(part * LANES, LANES), LANES)


def spectral_matrix(to, source, count):
    gap = (to[:, None] - source[None, :]) % count
    angle = gap.astype(jnp.float32) * (math.pi / count)
    parity = 1.0 - 2.0 * (gap % 2).astype(jnp.float32)
    divisor = jnp.where(gap == 0, 1.0, jnp.sin(angle))
    return jnp.where(gap == 0, 0.0, parity * jnp.cos(angle) / divisor * (2.0 / count))


def source_rows(y_sizes, place, row_depth, height):
    ends = jnp.cumsum(y_sizes)
    starts = ends - y_sizes
    cells = jnp.arange(height, dtype=jnp.int32)
    block = jnp.sum((cells[:, None] >= ends[None, :]).astype(jnp.int32), axis=1)
    stored = jnp.take(place, block) * row_depth + cells - jnp.take(starts, block)
    return stored


def row_exchange(value, split, concat):
    return lax.all_to_all(value, "row", split_axis=split, concat_axis=concat, tiled=True)


def col_exchange(value, split, concat):
    return lax.all_to_all(value, "col", split_axis=split, concat_axis=concat, tiled=True)


def on_device(velocity, y_sizes, old_place, new_col):
    saved = velocity
    velocity = velocity[:, 0]
    fields, places, row_depth, planes, x_cells = velocity.shape
    columns = lax.axis_size("col")
    rows_count = lax.axis_size("row")
    my_col = lax.axis_index("col")
    thick = planes // columns
    blocks_y = y_sizes.shape[0]
    height = YMEAN * blocks_y
    depth = planes * columns
    x_part = x_cells // rows_count
    y_part = height // columns
    slots = jnp.arange(columns, dtype=jnp.int32)
    hits = (new_col[:, :, None] == slots[None, None, :]).astype(jnp.int32)
    slab_of = jnp.sum(hits * slots[None, :, None], axis=1)

    stored = source_rows(y_sizes, jnp.take(old_place, my_col, axis=0), row_depth, height)
    pick = (stored[:, None] == jnp.arange(blocks_y * row_depth)[None, :]).astype(jnp.float32)
    cells = jnp.arange(height, dtype=jnp.int32)
    grid_row = jnp.sum(pick * cells[:, None].astype(jnp.float32), axis=0).astype(jnp.int32)
    used = jnp.sum(pick, axis=0)
    across_y = spectral_matrix(cells, grid_row, height) * used[None, :]
    steps_x = jnp.arange(x_cells, dtype=jnp.int32)
    across_x = spectral_matrix(steps_x, steps_x, x_cells)

    slope_x = jnp.dot(velocity[0], across_x.T, precision=FINE, preferred_element_type=jnp.float32)
    direct = x_part == LANES
    parted = (rows_count, places, row_depth, planes, x_part)
    pencil = parted[1:]
    slab = (columns, y_part, planes, x_part)
    whole = lambda ref, part: ref
    nth = lambda ref, part: ref.at[part]
    if direct:
        (third,) = exchange(
            0,
            [saved],
            [parted],
            [(0, 0, "row", lambda ref, part: ref.at[2, 0, :, :, :, lanes(part)], nth)],
            [pencil],
        )
    else:
        along_y = jnp.stack([slope_x, velocity[1]])
        two = row_exchange(along_y, 4, 1)
        third = row_exchange(velocity[2], 3, 0)
    third = third.reshape(blocks_y * row_depth, planes, x_part)
    upright = jnp.take(third, stored, axis=0)
    upright = upright.reshape(slab)
    if direct:
        first_part, second_part, upright = exchange(
            1,
            [upright, slope_x, saved],
            [parted, parted, slab],
            [
                (0, 2, "col", nth, nth),
                (1, 0, "row", lambda ref, part: ref.at[:, :, :, lanes(part)], nth),
                (2, 1, "row", lambda ref, part: ref.at[1, 0, :, :, :, lanes(part)], nth),
            ],
            [slab[1:], pencil, pencil],
        )
        two = [first_part, second_part]
    else:
        upright = col_exchange(upright, 0, 0)
    two = [one.reshape(blocks_y * row_depth, planes, x_part) for one in two]
    first = slots[None, :, None] * planes + slab_of.T[:, :, None] * thick
    targets = (first + jnp.arange(thick, dtype=jnp.int32)).reshape(-1)
    across_z = spectral_matrix(targets, jnp.arange(depth, dtype=jnp.int32), depth)
    slope_z = jnp.einsum(
        "akz,kyzx->ayx",
        across_z.reshape(depth, columns, planes),
        upright,
        precision=FINE,
    )
    slope_z = slope_z.reshape(columns, planes, y_part, x_part)
    flat = jnp.einsum("jy,yzx->zjx", across_y, two[1], precision=FINE)
    flat = flat + jnp.swapaxes(jnp.take(two[0], stored, axis=0), 0, 1)
    flat = flat.reshape(columns, thick, height, x_part)
    flat = jnp.take(flat, jnp.take(slab_of, my_col, axis=0), axis=0)
    if direct:
        flat, slope_z = exchange(
            2,
            [flat, slope_z],
            [(columns, thick, height, x_part), (planes, height, x_part)],
            [
                (0, 0, "col", nth, nth),
                (1, 1, "col", nth, lambda ref, part: ref.at[:, pl.ds(part * y_part, y_part), :]),
            ],
            [(thick, height, x_part), (planes, y_part, x_part)],
        )
        flat = flat.reshape(planes, height, x_part)
    else:
        flat = col_exchange(flat, 0, 0).reshape(planes, height, x_part)
        slope_z = col_exchange(slope_z, 0, 2).reshape(planes, height, x_part)
    part = flat + slope_z
    local_peak = jnp.max(jnp.abs(part), axis=0)
    per_row = columns // rows_count
    if direct:
        field, peaks = exchange(
            3,
            [part.reshape(rows_count, per_row, thick, height, x_part), local_peak],
            [(per_row, 1, thick, height, x_cells), (columns, height, x_part)],
            [
                (0, 0, "row", nth, lambda ref, part: ref.at[:, 0, :, :, lanes(part)]),
                (1, 1, "col", whole, nth),
            ],
            [(per_row, thick, height, x_part), (height, x_part)],
        )
        (peak,) = exchange(
            4,
            [jnp.max(peaks, axis=0)],
            [(height, x_cells)],
            [(0, 0, "row", whole, lambda ref, part: ref.at[:, lanes(part)])],
            [(height, x_part)],
        )
    else:
        peak = lax.pmax(local_peak, "col")
        peak = lax.all_gather(peak, "row", axis=1, tiled=True)
        field = row_exchange(part, 0, 2)
        field = field.reshape(per_row, 1, thick, height, x_cells)
    return (field, peak)


def solution(mesh):
    in_specs = (P(None, "col", "row", None, None, None), P(), P(), P())
    out_specs = (P("row", "col", None, None, None), P())
    return jax.shard_map(
        on_device, mesh=mesh, in_specs=in_specs, out_specs=out_specs, check_vma=False
    )
```
